32 devices in a mesh: slab: 8 (over z, x), sub: 4 (over y, core).
Axes of the slice: x: 2, y: 2, z: 4, core: 2. Of those that a mesh axis runs over, the one named last changes fastest.
Arguments:
- values: float32 [768, 2, 128, 256], P(('slab', 'sub')), may hold values from -0.25 to 0.25
- block_ids: int32 [768, 2], P(('slab', 'sub')), may hold values from 0 to 383, as said below
- tile_counts: int32 [8, 4], P('slab', 'sub'), may hold values from 8 to 24, as said below
- right_side: float32 [768, 128], P(('slab', 'sub')), may hold values from -18 to 18
Outputs:
- solution: float32 [384, 256], P(('slab', 'sub'))
- residual: float32 [768, 128], P(('slab', 'sub'))
The draws below stay inside these ranges and needn't reach their ends.
Inputs may be any that keep to these rules, and one draw needn't show every extreme that they name: `block_ids`: every block id names a node block held by a device of the row tile's own slab or of a slab one index of slab away; the first coupled block of each tile lies in its own slab. Block b is held by device b div 12. `tile_counts`: some device has all 24 slots live in every draw.
All inputs are finite; a program needn't handle non-finite values.
Results may differ from the reference program's by a relative error of at most 0.0003.
Values sent between devices are 32-bit elements; how exact they have to be, the bound alone decides.
No kernel may reach another device: no remote copies, remote signals or barrier semaphores. Data moves between devices by JAX's collectives and lax.ppermute only.
A program may use at most 64 MiB of HBM per device.

```python
import jax
import jax.numpy as jnp
from jax import lax

BLOCK = 256
TILE_ROWS = 128
COUPLED = 2
ITERS = 4
TILES_DEV = 24
NB_DEV = 12
TILES = 768
NBLOCKS = 384
N_SLAB = 8
N_SUB = 4


def draw_block_ids(key, part):
    tile_slab = jnp.arange(TILES, dtype=jnp.int32) // TILES_DEV // N_SUB
    offset = jax.random.randint(jax.random.fold_in(key, 11), (TILES, COUPLED), -1, 2)
    first_slot = jnp.arange(COUPLED, dtype=jnp.int32)[None, :] == 0
    offset = jnp.where(first_slot, 0, offset)
    other_slab = jnp.clip(tile_slab[:, None] + offset, 0, N_SLAB - 1)
    owner_sub = jax.random.randint(jax.random.fold_in(key, 12), (TILES, COUPLED), 0, N_SUB)
    slot_index = jax.random.randint(jax.random.fold_in(key, 13), (TILES, COUPLED), 0, NB_DEV)
    return ((other_slab * N_SUB + owner_sub) * NB_DEV + slot_index).astype(jnp.int32)


def draw_tile_counts(key, part):
    lowest = TILES_DEV // 3
    counts = jax.random.randint(jax.random.fold_in(key, 21), (N_SLAB * N_SUB,), lowest, TILES_DEV + 1)
    fuller = jax.random.randint(jax.random.fold_in(key, 22), (), 0, N_SLAB * N_SUB)
    counts = jnp.where(jnp.arange(N_SLAB * N_SUB, dtype=jnp.int32) == fuller, TILES_DEV, counts)
    return counts.reshape(N_SLAB, N_SUB).astype(jnp.int32)


def draw_right_side(key, part):
    position = jnp.arange(TILES, dtype=jnp.float32) / max(TILES - 1, 1)
    base = jnp.clip(jax.random.normal(jax.random.fold_in(key, 32), (TILES, TILE_ROWS), jnp.float32), -6.0, 6.0)
    rising = 1.0 + 2.0 * position
    return (base * rising[:, None]).astype(jnp.float32)


def steps_of(stream_key, extent, shards, smallest, top_value):
    level = 1.0
    for dim, parts in shards:
        heights = jax.random.uniform(jax.random.fold_in(jax.random.fold_in(stream_key, 6), dim), (parts,), jnp.float32, smallest / len(shards), top_value / len(shards))
        level = level * jnp.repeat(jnp.exp(heights), extent[dim] // parts).reshape((-1,) + (1,) * (len(extent) - 1 - dim))
    return level


def bell_draw(key, extent, width, reach, split=(), held_as=jnp.bfloat16):
    entries = jax.random.normal(key, extent, jnp.float32) * width
    if len(split) > 0:
        entries = steps_of(key, extent, split, -0.22, 0.18) * entries
    return jnp.clip(entries, min=-reach, max=reach).astype(held_as)


def setup_inputs(seed: int = 0) -> dict:
    key_list = jax.random.split(jax.random.key(seed), 5)
    return {
        "values": bell_draw(key_list[0], (TILES, COUPLED, TILE_ROWS, BLOCK), (COUPLED * BLOCK) ** -0.5, 0.25, ((0, 32),), jnp.float32),
        "block_ids": draw_block_ids(jax.random.fold_in(key_list[4], 71), 0),
        "tile_counts": draw_tile_counts(jax.random.fold_in(key_list[4], 71), 0),
        "right_side": draw_right_side(jax.random.fold_in(key_list[4], 71), 0),
    }


precise = lax.Precision.HIGHEST


def live_mask(tile_counts):
    position = jnp.arange(TILES, dtype=jnp.int32)
    owner_dev = (position // TILES_DEV).astype(jnp.int32)
    limit = tile_counts.reshape(-1)[owner_dev]
    return ((position % TILES_DEV) < limit).astype(jnp.float32)


def forward(values, block_ids, live_tiles, field):
    picked = field[block_ids]
    image = jnp.einsum("tkij,tkj->ti", values, picked, precision=precise)
    return image * live_tiles[:, None]


def backward(values, block_ids, rows):
    terms = jnp.einsum("tkij,ti->tkj", values, rows, precision=precise)
    return jax.ops.segment_sum(terms.reshape(-1, BLOCK), block_ids.reshape(-1), num_segments=NBLOCKS)


def reference(values, block_ids, tile_counts, right_side):
    live_tiles = live_mask(tile_counts)
    squares = jnp.einsum("tkij,tkij->tkj", values, values, precision=precise) * live_tiles[:, None, None]
    col_squares = jax.ops.segment_sum(squares.reshape(-1, BLOCK), block_ids.reshape(-1), num_segments=NBLOCKS)
    jacobi = 1.0 / (1.0 + col_squares)
    solution = jnp.zeros((NBLOCKS, BLOCK), jnp.float32)
    residual = right_side * live_tiles[:, None]
    normal_res = backward(values, block_ids, residual)
    scaled = jacobi * normal_res
    direction = scaled
    rho_now = jnp.sum(normal_res * scaled)
    for iteration in range(ITERS):
        image = forward(values, block_ids, live_tiles, direction)
        step_size = rho_now / jnp.sum(image * image)
        solution = solution + step_size * direction
        residual = residual - step_size * image
        normal_res = backward(values, block_ids, residual)
        scaled = jacobi * normal_res
        rho_next = jnp.sum(normal_res * scaled)
        direction = scaled + (rho_next / rho_now) * direction
        rho_now = rho_next
    return (solution, residual)
```

```python
import functools

import jax
import jax.numpy as jnp
from jax import lax
from jax.experimental import pallas as pl
from jax.experimental.pallas import tpu as pltpu
from jax.sharding import PartitionSpec as P

ITERS = 4
NB_DEV = 12
PART = -(-NB_DEV // 8) * 8
PIECE = 3 * PART
CHUNK = 4


def start_copies(values_ref, vbuf, sems):
    chunks = vbuf.shape[0] // CHUNK
    copies = []
    for c in range(chunks):
        copies.append(
            pltpu.make_async_copy(
                values_ref.at[pl.ds(c * CHUNK, CHUNK)], vbuf.at[pl.ds(c * CHUNK, CHUNK)], sems.at[c]
            )
        )
    for copy in copies:
        copy.start()
    return copies


def eye_mask(rows):
    return lax.broadcasted_iota(jnp.int32, (rows, rows), 0) == lax.broadcasted_iota(
        jnp.int32, (rows, rows), 1
    )


def live_of(count_ref, t):
    return jnp.where(t < count_ref[0, 0], 1.0, 0.0).astype(jnp.float32)


def first_kernel(rows_ref, count_ref, values_ref, right_ref, *refs, sub_count):
    pieces = refs[:sub_count]
    res_ref = refs[sub_count]
    vbuf, wbuf, sems = refs[sub_count + 1 :]
    copies = start_copies(values_ref, vbuf, sems)
    window = sub_count * PIECE
    wbuf[...] = jnp.zeros_like(wbuf)
    rows = vbuf.shape[2]
    eye = eye_mask(rows)
    for c, copy in enumerate(copies):
        copy.wait()
        for t in range(c * CHUNK, (c + 1) * CHUNK):
            live = live_of(count_ref, t)
            brow = right_ref[pl.ds(t, 1), :] * live
            res_ref[pl.ds(t, 1), :] = brow
            bcol = jnp.sum(jnp.where(eye, brow, 0.0), axis=1, keepdims=True)
            for k in range(vbuf.shape[1]):
                v = vbuf[t, k]
                row = rows_ref[t, k]
                wbuf[pl.ds(row, 1), :] += jnp.sum(v * bcol, axis=0, keepdims=True)
                wbuf[pl.ds(window + row, 1), :] += jnp.sum(v * v, axis=0, keepdims=True) * live
    for d in range(sub_count):
        pieces[d][0:PIECE, :] = wbuf[pl.ds(d * PIECE, PIECE), :]
        pieces[d][PIECE : 2 * PIECE, :] = wbuf[pl.ds(window + d * PIECE, PIECE), :]


def products(rows_ref, count_ref, copies, vbuf, zbuf, wbuf, u_ref):
    rows = vbuf.shape[2]
    half = vbuf.shape[3] // 2
    eye = eye_mask(rows)
    for c, copy in enumerate(copies):
        copy.wait()
        for t in range(c * CHUNK, (c + 1) * CHUNK):
            acc = None
            for k in range(vbuf.shape[1]):
                term = vbuf[t, k] * zbuf[pl.ds(rows_ref[t, k], 1), :]
                acc = term if acc is None else acc + term
            acc = acc[:, :half] + acc[:, half:]
            ucol = jnp.sum(acc, axis=1, keepdims=True) * live_of(count_ref, t)
            u_ref[pl.ds(t, 1), :] = jnp.sum(jnp.where(eye, ucol, 0.0), axis=0, keepdims=True)
            if wbuf is not None:
                for k in range(vbuf.shape[1]):
                    wbuf[pl.ds(rows_ref[t, k], 1), :] += jnp.sum(
                        vbuf[t, k] * ucol, axis=0, keepdims=True
                    )


def total(x):
    return jnp.sum(jnp.sum(x, axis=0, keepdims=True), axis=1, keepdims=True)


def put_sums(sums_ref, gamma, uu, uc):
    lane = lax.broadcasted_iota(jnp.int32, (1, 128), 1)
    line = jnp.where(lane == 0, gamma, jnp.where(lane == 1, uu, jnp.where(lane == 2, uc, 0.0)))
    sums_ref[...] = jnp.broadcast_to(line[None], sums_ref.shape)


def own_rows(ref):
    return ref[PART : PART + NB_DEV, :]


def second_kernel(rows_ref, count_ref, values_ref, *refs, sub_count):
    n = sub_count
    got = refs[:n]
    pieces = refs[n : 2 * n]
    r_ref, j_ref, z_ref, u_ref, sums_ref = refs[2 * n : 2 * n + 5]
    vbuf, wbuf, sems = refs[2 * n + 5 :]
    copies = start_copies(values_ref, vbuf, sems)
    for d in range(n):
        here = pl.ds(d * PIECE, PIECE)
        r = got[d][0:PIECE, :]
        jac = 1.0 / (1.0 + got[d][PIECE : 2 * PIECE, :])
        r_ref[here, :] = r
        j_ref[here, :] = jac
        z_ref[here, :] = jac * r
    wbuf[...] = jnp.zeros_like(wbuf)
    products(rows_ref, count_ref, copies, vbuf, z_ref, wbuf, u_ref)
    for d in range(n):
        pieces[d][...] = wbuf[pl.ds(d * PIECE, PIECE), :]
    u = u_ref[...]
    put_sums(sums_ref, total(own_rows(r_ref) * own_rows(z_ref)), total(u * u), 0.0)


def scalars_of(sums_ref, old_ref, first):
    line = jnp.sum(sums_ref[...], axis=0)[0:1, :]
    gamma, uu, uc = line[:, 0:1], line[:, 1:2], line[:, 2:3]
    if first:
        return gamma, uu, gamma / uu, None
    beta = gamma / old_ref[0:1, 0:1]
    norm = uu + 2.0 * beta * uc + beta * beta * old_ref[0:1, 1:2]
    return gamma, norm, gamma / norm, beta


def middle_kernel(rows_ref, count_ref, values_ref, *refs, sub_count, first, last):
    n = sub_count
    got, refs = refs[:n], refs[n:]
    sums_in, r_in, j_in, z_in, u_in, res_in = refs[:6]
    refs = refs[6:]
    d_in = q_in = image_in = x_in = old_in = None
    if not first:
        d_in, q_in, image_in, x_in, old_in = refs[:5]
        refs = refs[5:]
    pieces = None
    if not last:
        pieces, refs = refs[:n], refs[n:]
    r_ref, z_ref, u_ref, res_ref, d_ref, q_ref, image_ref, x_ref, old_ref, sums_ref = refs[:10]
    vbuf, wbuf, sems = refs[10:]
    copies = start_copies(values_ref, vbuf, sems)
    gamma, norm, step, beta = scalars_of(sums_in, old_in, first)
    lane = lax.broadcasted_iota(jnp.int32, (8, 128), 1)
    old_ref[...] = jnp.where(lane == 0, gamma, norm)
    for d in range(n):
        here = pl.ds(d * PIECE, PIECE)
        q = got[d][...]
        direction = z_in[here, :]
        if not first:
            q = q + beta * q_in[here, :]
            direction = direction + beta * d_in[here, :]
        r = r_in[here, :] - step * q
        r_ref[here, :] = r
        z_ref[here, :] = j_in[here, :] * r
        q_ref[here, :] = q
        d_ref[here, :] = direction
    wbuf[...] = jnp.zeros_like(wbuf)
    image = u_in[...]
    if not first:
        image = image + beta * image_in[...]
    image_ref[...] = image
    res_ref[...] = res_in[...] - step * image
    moved = step * own_rows(d_ref)
    x_ref[...] = moved if first else x_in[...] + moved
    products(rows_ref, count_ref, copies, vbuf, z_ref, None if last else wbuf, u_ref)
    if not last:
        for d in range(n):
            pieces[d][...] = wbuf[pl.ds(d * PIECE, PIECE), :]
    u = u_ref[...]
    put_sums(sums_ref, total(own_rows(r_ref) * own_rows(z_ref)), total(u * u), total(u * image))


def final_kernel(sums_in, z_in, u_in, res_in, d_in, image_in, x_in, old_in, x_ref, res_ref):
    _, _, step, beta = scalars_of(sums_in, old_in, False)
    x_ref[...] = x_in[...] + step * (own_rows(z_in) + beta * own_rows(d_in))
    res_ref[...] = res_in[...] - step * (u_in[...] + beta * image_in[...])


def per_device(values, block_ids, tile_counts, right_side):
    tiles_dev, coupled, tile_rows, block_len = values.shape
    sub_count = lax.axis_size("sub")
    slab_count = lax.axis_size("slab")
    devices = sub_count * slab_count
    slab_index = lax.axis_index("slab")
    sub_index = lax.axis_index("sub")
    owner_dev = block_ids // NB_DEV
    rel_slab = owner_dev // sub_count - slab_index + 1
    rel_sub = (owner_dev % sub_count - sub_index + sub_count) % sub_count
    rows = rel_sub * PIECE + rel_slab * PART + block_ids % NB_DEV

    window = sub_count * PIECE
    f32 = jnp.float32
    piece = jax.ShapeDtypeStruct((PIECE, block_len), f32)
    field = jax.ShapeDtypeStruct((window, block_len), f32)
    row_field = jax.ShapeDtypeStruct((tiles_dev, tile_rows), f32)
    sums = jax.ShapeDtypeStruct((devices, 8, 128), f32)
    own = jax.ShapeDtypeStruct((NB_DEV, block_len), f32)
    old = jax.ShapeDtypeStruct((8, 128), f32)
    smem = pl.BlockSpec(memory_space=pltpu.SMEM)
    vmem = pl.BlockSpec(memory_space=pltpu.VMEM)
    hbm = pl.BlockSpec(memory_space=pl.ANY)

    def call(kernel, name, inputs, outs, wrows):
        return pl.pallas_call(
            kernel,
            name=name,
            in_specs=[smem, smem, hbm] + [vmem] * len(inputs),
            out_specs=[vmem] * len(outs),
            out_shape=outs,
            scratch_shapes=[
                pltpu.VMEM(values.shape, f32),
                pltpu.VMEM((wrows, block_len), f32),
                pltpu.SemaphoreType.DMA((tiles_dev // CHUNK,)),
            ],
            compiler_params=pltpu.CompilerParams(vmem_limit_bytes=24 * 1024 * 1024),
        )(rows, tile_counts, values, *inputs)

    def shift(block, axis, distance, wrap):
        count = lax.axis_size(axis)
        route = [
            (i, (i + distance) % count) for i in range(count) if wrap or 0 <= i + distance < count
        ]
        return lax.ppermute(block, axis, route)

    def exchange(pieces):
        width = pieces[0].shape[0] // PIECE
        moved = [shift(pieces[d], "sub", d, True) for d in range(1, sub_count)]
        mine = pieces[0]
        for block in moved:
            mine = mine + block
        mine = mine.reshape(width, 3, PART, block_len)
        low_one = shift(mine[:, 1:3], "slab", 1, False)
        high_one = shift(mine[:, 0:2], "slab", -1, False)
        low_two = shift(mine[:, 2:3], "slab", 2, False)
        high_two = shift(mine[:, 0:1], "slab", -2, False)
        summed = jnp.concatenate(
            [
                mine[:, 0:1] + low_one[:, 0:1] + low_two,
                mine[:, 1:2] + low_one[:, 1:2] + high_one[:, 0:1],
                mine[:, 2:3] + high_one[:, 1:2] + high_two,
            ],
            axis=1,
        ).reshape(width * PIECE, block_len)
        return [summed] + [shift(summed, "sub", -d, True) for d in range(1, sub_count)]

    def spread(local):
        return lax.all_to_all(local, ("slab", "sub"), 0, 0, tiled=True)

    outs = call(
        functools.partial(first_kernel, sub_count=sub_count),
        "cgls_first",
        [right_side],
        [jax.ShapeDtypeStruct((2 * PIECE, block_len), f32)] * sub_count + [row_field],
        2 * window,
    )
    got = exchange(outs[:sub_count])
    residual = outs[sub_count]
    outs = call(
        functools.partial(second_kernel, sub_count=sub_count),
        "cgls_second",
        got,
        [piece] * sub_count + [field, field, field, row_field, sums],
        window,
    )
    pieces = outs[:sub_count]
    normal_res, jacobi, scaled, image_part, local_sums = outs[sub_count:]
    carried = []
    for iteration in range(ITERS - 1):
        first, last = iteration == 0, iteration == ITERS - 2
        all_sums = spread(local_sums)
        got = exchange(pieces)
        outs = call(
            functools.partial(middle_kernel, sub_count=sub_count, first=first, last=last),
            "cgls_middle",
            list(got) + [all_sums, normal_res, jacobi, scaled, image_part, residual] + carried,
            ([] if last else [piece] * sub_count)
            + [field, field, row_field, row_field, field, field, row_field, own, old, sums],
            window,
        )
        if not last:
            pieces, outs = outs[:sub_count], outs[sub_count:]
        normal_res, scaled, image_part, residual, direction, back, image, x, seen, local_sums = outs
        carried = [direction, back, image, x, seen]
    all_sums = spread(local_sums)
    return tuple(
        pl.pallas_call(
            final_kernel,
            name="cgls_final",
            in_specs=[vmem] * 8,
            out_specs=[vmem] * 2,
            out_shape=[own, row_field],
            compiler_params=pltpu.CompilerParams(vmem_limit_bytes=16 * 1024 * 1024),
        )(all_sums, scaled, image_part, residual, direction, image, x, seen)
    )


def solution(mesh):
    in_specs = (
        P(("slab", "sub"), None, None, None),
        P(("slab", "sub"), None),
        P("slab", "sub"),
        P(("slab", "sub"), None),
    )
    out_specs = (P(("slab", "sub"), None), P(("slab", "sub"), None))
    return jax.shard_map(
        per_device, mesh=mesh, in_specs=in_specs, out_specs=out_specs, check_vma=False
    )
```

```python
import functools

import jax
import jax.numpy as jnp
from jax import lax
from jax.experimental import pallas as pl
from jax.experimental.pallas import tpu as pltpu
from jax.sharding import PartitionSpec as P

ITERS = 4
NB_DEV = 12
PART = -(-NB_DEV // 8) * 8
PIECE = 3 * PART
CHUNK = 4


def start_copies(values_ref, vbuf, sems):
    copies = []
    for c in range(vbuf.shape[0] // CHUNK):
        part = pl.ds(c * CHUNK, CHUNK)
        copies.append(pltpu.make_async_copy(values_ref.at[part], vbuf.at[part], sems.at[c]))
    for copy in copies:
        copy.start()
    return copies


def eye_mask(rows):
    return lax.broadcasted_iota(jnp.int32, (rows, rows), 0) == lax.broadcasted_iota(
        jnp.int32, (rows, rows), 1
    )


def live_of(count_ref, t):
    return jnp.where(t < count_ref[0, 0], 1.0, 0.0).astype(jnp.float32)


def window_row(block, slab_index, sub_index, sub_count):
    owner = lax.div(block, jnp.int32(NB_DEV))
    slab = lax.div(owner, jnp.int32(sub_count))
    rel_sub = lax.bitwise_xor(owner - slab * sub_count, sub_index)
    return rel_sub * PIECE + (slab - slab_index + 1) * PART + block - owner * NB_DEV


def first_kernel(ids_ref, count_ref, place_ref, values_ref, right_ref, *refs, sub_count):
    pieces = refs[:sub_count]
    res_ref, rows_ref = refs[sub_count : sub_count + 2]
    vbuf, wbuf, sems = refs[sub_count + 2 :]
    copies = start_copies(values_ref, vbuf, sems)
    window = sub_count * PIECE
    wbuf[...] = jnp.zeros_like(wbuf)
    rows = vbuf.shape[2]
    eye = eye_mask(rows)
    for c, copy in enumerate(copies):
        copy.wait()
        for t in range(c * CHUNK, (c + 1) * CHUNK):
            live = live_of(count_ref, t)
            brow = right_ref[pl.ds(t, 1), :] * live
            res_ref[pl.ds(t, 1), :] = brow
            bcol = jnp.sum(jnp.where(eye, brow, 0.0), axis=1, keepdims=True)
            for k in range(vbuf.shape[1]):
                v = vbuf[t, k]
                row = window_row(ids_ref[t, k], place_ref[0, 0], place_ref[0, 1], sub_count)
                rows_ref[t, k] = row
                wbuf[pl.ds(row, 1), :] += jnp.sum(v * bcol, axis=0, keepdims=True)
                wbuf[pl.ds(window + row, 1), :] += jnp.sum(v * v, axis=0, keepdims=True) * live
    for d in range(sub_count):
        pieces[d][0:PIECE, :] = wbuf[pl.ds(d * PIECE, PIECE), :]
        pieces[d][PIECE : 2 * PIECE, :] = wbuf[pl.ds(window + d * PIECE, PIECE), :]


def products(rows_ref, count_ref, copies, vbuf, zbuf, wbuf, u_ref):
    rows = vbuf.shape[2]
    half = vbuf.shape[3] // 2
    eye = eye_mask(rows)
    for t in range(vbuf.shape[0]):
        if t % CHUNK == 0:
            copies[t // CHUNK].wait()
        acc = None
        for k in range(vbuf.shape[1]):
            term = vbuf[t, k] * zbuf[pl.ds(rows_ref[t, k], 1), :]
            acc = term if acc is None else acc + term
        acc = acc[:, :half] + acc[:, half:]
        ucol = jnp.sum(acc, axis=1, keepdims=True) * live_of(count_ref, t)
        u_ref[pl.ds(t, 1), :] = jnp.sum(jnp.where(eye, ucol, 0.0), axis=0, keepdims=True)
        if wbuf is not None:
            for k in range(vbuf.shape[1]):
                wbuf[pl.ds(rows_ref[t, k], 1), :] += jnp.sum(
                    vbuf[t, k] * ucol, axis=0, keepdims=True
                )


def total(x):
    return jnp.sum(jnp.sum(x, axis=0, keepdims=True), axis=1, keepdims=True)


def put_sums(sums_ref, gamma, uu, uc):
    lane = lax.broadcasted_iota(jnp.int32, (1, 128), 1)
    line = jnp.where(lane == 0, gamma, jnp.where(lane == 1, uu, jnp.where(lane == 2, uc, 0.0)))
    sums_ref[...] = jnp.broadcast_to(line[None], sums_ref.shape)


def own_rows(ref):
    return ref[PART : PART + NB_DEV, :]


def second_kernel(rows_ref, count_ref, values_ref, *refs, sub_count):
    n = sub_count
    got = refs[:n]
    pieces = refs[n : 2 * n]
    r_ref, j_ref, z_ref, u_ref, sums_ref = refs[2 * n : 2 * n + 5]
    vbuf, wbuf, sems = refs[2 * n + 5 :]
    copies = start_copies(values_ref, vbuf, sems)
    for d in range(n):
        here = pl.ds(d * PIECE, PIECE)
        r = got[d][0:PIECE, :]
        jac = 1.0 / (1.0 + got[d][PIECE : 2 * PIECE, :])
        r_ref[here, :] = r
        j_ref[here, :] = jac
        z_ref[here, :] = jac * r
    wbuf[...] = jnp.zeros_like(wbuf)
    products(rows_ref, count_ref, copies, vbuf, z_ref, wbuf, u_ref)
    for d in range(n):
        pieces[d][...] = wbuf[pl.ds(d * PIECE, PIECE), :]
    u = u_ref[...]
    put_sums(sums_ref, total(own_rows(r_ref) * own_rows(z_ref)), total(u * u), 0.0)


def scalars_of(sums_ref, old_ref, first):
    line = jnp.sum(sums_ref[...], axis=0)[0:1, :]
    gamma, uu, uc = line[:, 0:1], line[:, 1:2], line[:, 2:3]
    if first:
        return gamma, uu, gamma / uu, None
    beta = gamma / old_ref[0:1, 0:1]
    norm = uu + 2.0 * beta * uc + beta * beta * old_ref[0:1, 1:2]
    return gamma, norm, gamma / norm, beta


def middle_kernel(rows_ref, count_ref, values_ref, *refs, sub_count, first, last):
    n = sub_count
    got, refs = refs[:n], refs[n:]
    sums_in, r_in, j_in, z_in, u_in, res_in = refs[:6]
    refs = refs[6:]
    d_in = q_in = image_in = x_in = old_in = None
    if not first:
        d_in, q_in, image_in, x_in, old_in = refs[:5]
        refs = refs[5:]
    pieces = None
    if not last:
        pieces, refs = refs[:n], refs[n:]
    r_ref, z_ref, u_ref, res_ref, d_ref, q_ref, image_ref, x_ref, old_ref, sums_ref = refs[:10]
    vbuf, wbuf, sems = refs[10:]
    copies = start_copies(values_ref, vbuf, sems)
    gamma, norm, step, beta = scalars_of(sums_in, old_in, first)
    lane = lax.broadcasted_iota(jnp.int32, (8, 128), 1)
    old_ref[...] = jnp.where(lane == 0, gamma, norm)
    for d in range(n):
        here = pl.ds(d * PIECE, PIECE)
        q = got[d][...]
        direction = z_in[here, :]
        if not first:
            q = q + beta * q_in[here, :]
            direction = direction + beta * d_in[here, :]
        r = r_in[here, :] - step * q
        r_ref[here, :] = r
        z_ref[here, :] = j_in[here, :] * r
        q_ref[here, :] = q
        d_ref[here, :] = direction
    wbuf[...] = jnp.zeros_like(wbuf)
    image = u_in[...]
    if not first:
        image = image + beta * image_in[...]
    image_ref[...] = image
    res_ref[...] = res_in[...] - step * image
    moved = step * own_rows(d_ref)
    x_ref[...] = moved if first else x_in[...] + moved
    products(rows_ref, count_ref, copies, vbuf, z_ref, None if last else wbuf, u_ref)
    if not last:
        for d in range(n):
            pieces[d][...] = wbuf[pl.ds(d * PIECE, PIECE), :]
    u = u_ref[...]
    put_sums(sums_ref, total(own_rows(r_ref) * own_rows(z_ref)), total(u * u), total(u * image))


def final_kernel(sums_in, z_in, u_in, res_in, d_in, image_in, x_in, old_in, x_ref, res_ref):
    _, _, step, beta = scalars_of(sums_in, old_in, False)
    x_ref[...] = x_in[...] + step * (own_rows(z_in) + beta * own_rows(d_in))
    res_ref[...] = res_in[...] - step * (u_in[...] + beta * image_in[...])


def per_device(values, block_ids, tile_counts, right_side):
    tiles_dev, coupled, tile_rows, block_len = values.shape
    sub_count = lax.axis_size("sub")
    slab_count = lax.axis_size("slab")
    devices = sub_count * slab_count
    slab_index = lax.axis_index("slab")
    sub_index = lax.axis_index("sub")
    place = jnp.stack([slab_index, sub_index]).astype(jnp.int32).reshape(1, 2)

    window = sub_count * PIECE
    f32 = jnp.float32
    piece = jax.ShapeDtypeStruct((PIECE, block_len), f32)
    field = jax.ShapeDtypeStruct((window, block_len), f32)
    row_field = jax.ShapeDtypeStruct((tiles_dev, tile_rows), f32)
    sums = jax.ShapeDtypeStruct((devices, 8, 128), f32)
    own = jax.ShapeDtypeStruct((NB_DEV, block_len), f32)
    old = jax.ShapeDtypeStruct((8, 128), f32)
    smem = pl.BlockSpec(memory_space=pltpu.SMEM)
    vmem = pl.BlockSpec(memory_space=pltpu.VMEM)
    hbm = pl.BlockSpec(memory_space=pltpu.HBM)
    limit = pltpu.CompilerParams(vmem_limit_bytes=48 * 1024 * 1024)

    def call(kernel, name, inputs, outs):
        return pl.pallas_call(
            kernel,
            name=name,
            in_specs=[smem, smem, hbm] + [vmem] * len(inputs),
            out_specs=[vmem] * len(outs),
            out_shape=outs,
            scratch_shapes=[
                pltpu.VMEM(values.shape, f32),
                pltpu.VMEM((window, block_len), f32),
                pltpu.SemaphoreType.DMA((tiles_dev // CHUNK,)),
            ],
            compiler_params=limit,
        )(rows, tile_counts, values, *inputs)

    def swap(block, axis, pairs):
        partner = {i: i for i in range(lax.axis_size(axis))}
        for a, b in pairs:
            partner[a], partner[b] = b, a
        return lax.ppermute(block, axis, list(partner.items()))

    def swap_sub(block, d):
        return swap(block, "sub", [(i, i ^ d) for i in range(sub_count) if i < i ^ d])

    def swap_slab(block, distance, offset):
        starts = [i for i in range(slab_count - distance) if (i // distance) % 2 == offset]
        pairs = [(i, i + distance) for i in starts]
        idle = [i for i in range(slab_count) if all(i not in pair for pair in pairs)]
        pairs += list(zip(idle[0::2], idle[1::2]))
        return swap(block, "slab", pairs)

    even_one = slab_index % 2 == 0
    even_two = slab_index // 2 % 2 == 0
    has_above, has_below = slab_index < slab_count - 1, slab_index > 0
    has_over, has_under = slab_index < slab_count - 2, slab_index > 1

    def exchange(pieces):
        width = pieces[0].shape[0] // PIECE
        mine = pieces[0]
        for block in [swap_sub(pieces[d], d) for d in range(1, sub_count)]:
            mine = mine + block
        mine = mine.reshape(width, 3, PART, block_len)
        to_above, to_below = mine[:, 1:3], mine[:, 0:2]
        far_above, far_below = mine[:, 2:3], mine[:, 0:1]
        near_a = swap_slab(jnp.where(even_one, to_above, to_below), 1, 0)
        near_b = swap_slab(jnp.where(even_one, to_below, to_above), 1, 1)
        far_a = swap_slab(jnp.where(even_two, far_above, far_below), 2, 0)
        far_b = swap_slab(jnp.where(even_two, far_below, far_above), 2, 1)
        above = jnp.where(has_above, jnp.where(even_one, near_a, near_b), 0.0)
        below = jnp.where(has_below, jnp.where(even_one, near_b, near_a), 0.0)
        over = jnp.where(has_over, jnp.where(even_two, far_a, far_b), 0.0)
        under = jnp.where(has_under, jnp.where(even_two, far_b, far_a), 0.0)
        summed = jnp.concatenate(
            [
                mine[:, 0:1] + below[:, 0:1] + under,
                mine[:, 1:2] + below[:, 1:2] + above[:, 0:1],
                mine[:, 2:3] + above[:, 1:2] + over,
            ],
            axis=1,
        ).reshape(width * PIECE, block_len)
        return [summed] + [swap_sub(summed, d) for d in range(1, sub_count)]

    def spread(local):
        return lax.all_to_all(local, ("slab", "sub"), 0, 0, tiled=True)

    outs = pl.pallas_call(
        functools.partial(first_kernel, sub_count=sub_count),
        name="cgls_first",
        in_specs=[smem, smem, smem, hbm, vmem],
        out_specs=[vmem] * (sub_count + 1) + [smem],
        out_shape=[jax.ShapeDtypeStruct((2 * PIECE, block_len), f32)] * sub_count
        + [
            row_field,
            jax.ShapeDtypeStruct(block_ids.shape, jnp.int32),
        ],
        scratch_shapes=[
            pltpu.VMEM(values.shape, f32),
            pltpu.VMEM((2 * window, block_len), f32),
            pltpu.SemaphoreType.DMA((tiles_dev // CHUNK,)),
        ],
        compiler_params=limit,
    )(block_ids, tile_counts, place, values, right_side)
    residual, rows = outs[sub_count:]
    got = exchange(outs[:sub_count])
    outs = call(
        functools.partial(second_kernel, sub_count=sub_count),
        "cgls_second",
        got,
        [piece] * sub_count + [field, field, field, row_field, sums],
    )
    pieces = outs[:sub_count]
    normal_res, jacobi, scaled, image_part, local_sums = outs[sub_count:]
    carried = []
    for iteration in range(ITERS - 1):
        first, last = iteration == 0, iteration == ITERS - 2
        all_sums = spread(local_sums)
        got = exchange(pieces)
        outs = call(
            functools.partial(middle_kernel, sub_count=sub_count, first=first, last=last),
            "cgls_middle",
            list(got) + [all_sums, normal_res, jacobi, scaled, image_part, residual] + carried,
            ([] if last else [piece] * sub_count)
            + [field, field, row_field, row_field, field, field, row_field, own, old, sums],
        )
        if not last:
            pieces, outs = outs[:sub_count], outs[sub_count:]
        normal_res, scaled, image_part, residual, direction, back, image, x, seen, local_sums = outs
        carried = [direction, back, image, x, seen]
    all_sums = spread(local_sums)
    return tuple(
        pl.pallas_call(
            final_kernel,
            name="cgls_final",
            in_specs=[vmem] * 8,
            out_specs=[vmem] * 2,
            out_shape=[own, row_field],
            compiler_params=limit,
        )(all_sums, scaled, image_part, residual, direction, image, x, seen)
    )


def solution(mesh):
    in_specs = (
        P(("slab", "sub"), None, None, None),
        P(("slab", "sub"), None),
        P("slab", "sub"),
        P(("slab", "sub"), None),
    )
    out_specs = (P(("slab", "sub"), None), P(("slab", "sub"), None))
    return jax.shard_map(
        per_device, mesh=mesh, in_specs=in_specs, out_specs=out_specs, check_vma=False
    )
```
